32 devices in a mesh: gx: 4 (over z), gy: 2 (over x), gz: 4 (over y, core).
Axes of the slice: x: 2, y: 2, z: 4, core: 2. Of those that a mesh axis runs over, the one named last changes fastest.
Arguments:
- old_slots: bfloat16 [4, 2, 32, 4096], P('gx', 'gy', 'gz'), may hold values from -6 to 6
- old_ids: int32 [4, 2, 32], P('gx', 'gy', 'gz'), may hold values from -1 to 31, as said below
- old_owner: int32 [4, 2, 32], P('gx', 'gy'), may hold values from 0 to 3, as said below
- coefficient: float32 [64, 32, 512], P('gx', 'gy', 'gz'), may hold values from 0.2 to 5
Outputs:
- solution: float32 [64, 32, 512], P('gx', 'gy', 'gz')
The draws below stay inside these ranges and needn't reach their ends.
Inputs may be any that keep to these rules, and one draw needn't show every extreme that they name: old_owner[a, c, b] is the index along gz of the device that held box b of box column (a, c) before the move; no device holds more than 8 boxes of a column and some device holds exactly 8; no device holds more than 2 of the 8 boxes with one value of b // 8, and that bound is reached. old_ids[a, c, g * 8 + q] is the box held in slot q of device g of box column (a, c), or -1 for an empty slot; it agrees with old_owner and each box stands in exactly one slot.
All inputs are finite; a program needn't handle non-finite values.
Results may differ from the reference program's by a relative error of at most 0.0003.
Values may be sent and summed in bfloat16 or wider, within the bound.
A program may use at most 64 MiB of HBM per device.

```python
import math
import jax
import jax.numpy as jnp
from jax import lax

BOX = 16
NB = 8
SWEEPS = 2
CAP = 8
NX = 64
NY = 32
NZ = 512
N_GX = 4
N_GY = 2
N_GZ = 4


def column_maps(column_key):
    groups = N_GZ
    halves = NB // 2
    pair_count = groups * halves
    subkeys = jax.random.split(column_key, 5)
    labels = jnp.arange(groups, dtype=jnp.int32)
    if NB <= groups:
        counts = jnp.where(labels < groups // 4, 2 * halves, jnp.where(labels < groups // 2, halves, halves // 2)).astype(jnp.int32)
    else:
        counts = jnp.full((groups,), halves, jnp.int32)
    ending = jnp.cumsum(counts).astype(jnp.int32)
    items = jnp.arange(pair_count, dtype=jnp.int32)
    sorted_owner = jnp.sum((items[:, None] >= ending[None, :]).astype(jnp.int32), axis=1)
    relabel = jax.random.permutation(subkeys[0], groups).astype(jnp.int32)
    item_owner = relabel[sorted_owner]
    columns = jax.random.permutation(subkeys[1], groups).astype(jnp.int32)
    target = columns[items % groups]
    levels = items // groups
    placing = jax.vmap(lambda single: jax.random.permutation(single, NB).astype(jnp.int32))(jax.random.split(subkeys[2], groups))
    first_box = target * NB + placing[target, 2 * levels]
    second_box = target * NB + placing[target, 2 * levels + 1]
    box_count = groups * NB
    owners = jnp.zeros((box_count,), jnp.int32).at[first_box].set(item_owner).at[second_box].set(item_owner)
    priority = jax.random.permutation(subkeys[3], box_count).astype(jnp.int32)
    sharing = owners[:, None] == owners[None, :]
    ranking = jnp.sum((sharing & (priority[None, :] < priority[:, None])).astype(jnp.int32), axis=1)
    offsets = jax.random.randint(subkeys[4], (groups,), 0, CAP, dtype=jnp.int32)
    slot_index = (ranking + offsets[owners]) % CAP
    slot_ids = jnp.full((groups * CAP,), -1, jnp.int32).at[owners * CAP + slot_index].set(jnp.arange(box_count, dtype=jnp.int32))
    return (owners, slot_ids)


def all_columns(key):
    column_keys = jax.random.split(jax.random.fold_in(key, 31), N_GX * N_GY)
    return jax.vmap(column_maps)(column_keys)


def draw_old_owner(key, part):
    owners, slot_ids = all_columns(key)
    return owners.reshape(N_GX, N_GY, N_GZ * NB)


def draw_old_ids(key, part):
    owners, slot_ids = all_columns(key)
    return slot_ids.reshape(N_GX, N_GY, N_GZ * CAP)


def draw_old_slots(key, part):
    shape = (N_GX, N_GY, N_GZ * CAP, BOX ** 3)
    noise_key = jax.random.fold_in(jax.random.fold_in(key, 47), 0)
    return jnp.clip(jax.random.normal(noise_key, shape, jnp.float32), -6.0, 6.0).astype(jnp.bfloat16)


def level_of(own_key, extent, cuts, low, largest):
    gain, own = 1.0, jax.random.fold_in(own_key, 6)
    for axis_at, shards_of in cuts:
        draws = jnp.exp(jax.random.uniform(jax.random.fold_in(own, axis_at), (shards_of,), jnp.float32, low / len(cuts), largest / len(cuts)))
        gain = gain * jnp.repeat(draws, extent[axis_at] // shards_of).reshape([-1 if axis == axis_at else 1 for axis in range(len(extent))])
    return gain


def setup_inputs(seed: int = 0) -> dict:
    key_list = jax.random.split(jax.random.key(seed), 5)
    return {
        "old_slots": draw_old_slots(jax.random.fold_in(key_list[4], 71), 0),
        "old_ids": draw_old_ids(jax.random.fold_in(key_list[4], 71), 0),
        "old_owner": draw_old_owner(jax.random.fold_in(key_list[4], 71), 0),
        "coefficient": jnp.clip(jnp.exp(math.log(5.0) - 3.218876 * jax.random.uniform(key_list[3], (NX, NY, NZ), jnp.float32) ** level_of(key_list[3], (NX, NY, NZ), ((0, 4), (1, 2), (2, 4)), -0.2, 0.2)), 0.2, 5.0),
    }


def inner(padded):
    return padded[1:-1, 1:-1, 1:-1]


def operator_parts(padded):
    face_first = 0.5 * (padded[:-1, 1:-1, 1:-1] + padded[1:, 1:-1, 1:-1])
    face_second = 0.5 * (padded[1:-1, :-1, 1:-1] + padded[1:-1, 1:, 1:-1])
    face_third = 0.5 * (padded[1:-1, 1:-1, :-1] + padded[1:-1, 1:-1, 1:])
    diagonal = face_first[:-1] + face_first[1:] + face_second[:, :-1] + face_second[:, 1:] + face_third[:, :, :-1] + face_third[:, :, 1:]
    return face_first, face_second, face_third, diagonal


def neighbours(padded, stencil):
    face_first, face_second, face_third, diagonal = stencil
    summed = face_first[:-1] * padded[:-2, 1:-1, 1:-1] + face_first[1:] * padded[2:, 1:-1, 1:-1]
    summed = summed + face_second[:, :-1] * padded[1:-1, :-2, 1:-1] + face_second[:, 1:] * padded[1:-1, 2:, 1:-1]
    summed = summed + face_third[:, :, :-1] * padded[1:-1, 1:-1, :-2] + face_third[:, :, 1:] * padded[1:-1, 1:-1, 2:]
    return summed


def red_cells(shape, margin):
    index_first = lax.broadcasted_iota(jnp.int32, shape, 0)
    index_second = lax.broadcasted_iota(jnp.int32, shape, 1)
    index_third = lax.broadcasted_iota(jnp.int32, shape, 2)
    return (index_first + index_second + index_third + margin) % 2 == 0


def relax(padded, source, stencil, factor, chosen):
    fresh = (factor * source + neighbours(padded, stencil)) / stencil[3]
    return jnp.where(chosen, fresh, inner(padded))


def apply_operator(values, stencil, factor):
    return (stencil[3] * values - neighbours(jnp.pad(values, 1), stencil)) / factor


def smooth(values, source, stencil, factor):
    red_mask = red_cells(source.shape, 0)
    black_mask = jnp.logical_not(red_mask)
    for counter in range(SWEEPS):
        values = relax(jnp.pad(values, 1), source, stencil, factor, red_mask)
        values = relax(jnp.pad(values, 1), source, stencil, factor, black_mask)
    return values


def coarsen(values):
    extent_first, extent_second, extent_third = values.shape
    grouped = values.reshape(extent_first // 2, 2, extent_second // 2, 2, extent_third // 2, 2)
    return grouped.mean(axis=(1, 3, 5))


def refine(values):
    return jnp.repeat(jnp.repeat(jnp.repeat(values, 2, axis=0), 2, axis=1), 2, axis=2)


def bicgstab(rhs_low, stencil, factor):
    image_low = apply_operator(rhs_low, stencil, factor)
    alpha_step = jnp.sum(rhs_low * rhs_low) / jnp.sum(rhs_low * image_low)
    rest_low = rhs_low - alpha_step * image_low
    turned = apply_operator(rest_low, stencil, factor)
    omega_step = jnp.sum(turned * rest_low) / jnp.sum(turned * turned)
    return alpha_step * rhs_low + omega_step * rest_low


def move_boxes(old_slots, old_ids, old_owner):
    column_boxes = NB * N_GZ
    held = old_ids.reshape(N_GX, N_GY, N_GZ, CAP)
    owner_index = jnp.broadcast_to(old_owner[:, :, :, None], (N_GX, N_GY, column_boxes, CAP))
    owner_slots = jnp.take_along_axis(held, owner_index, axis=2)
    wanted = jnp.arange(column_boxes, dtype=jnp.int32)
    position = jnp.argmax(owner_slots == wanted[None, None, :, None], axis=3).astype(jnp.int32)
    global_slot = old_owner * CAP + position
    picked = jax.vmap(jax.vmap(lambda stacked, chosen_rows: stacked[chosen_rows]))(old_slots, global_slot)
    boxes = picked.reshape(N_GX, N_GY, column_boxes, BOX, BOX, BOX).transpose(0, 3, 1, 4, 2, 5)
    return boxes.reshape(N_GX * BOX, N_GY * BOX, column_boxes * BOX)


def reference(old_slots, old_ids, old_owner, coefficient):
    source_fine = move_boxes(old_slots, old_ids, old_owner).astype(jnp.float32)
    stencil_fine = operator_parts(jnp.pad(coefficient, 1))
    fine_values = smooth(jnp.zeros_like(source_fine), source_fine, stencil_fine, 1.0)
    residual_fine = source_fine - apply_operator(fine_values, stencil_fine, 1.0)
    coefficient_mid = coarsen(coefficient)
    stencil_mid = operator_parts(jnp.pad(coefficient_mid, 1))
    source_mid = coarsen(residual_fine)
    middle_values = smooth(jnp.zeros_like(source_mid), source_mid, stencil_mid, 4.0)
    residual_mid = source_mid - apply_operator(middle_values, stencil_mid, 4.0)
    coefficient_low = coarsen(coefficient_mid)
    stencil_low = operator_parts(jnp.pad(coefficient_low, 1))
    bottom_values = bicgstab(coarsen(residual_mid), stencil_low, 16.0)
    middle_values = smooth(middle_values + refine(bottom_values), source_mid, stencil_mid, 4.0)
    return smooth(fine_values + refine(middle_values), source_fine, stencil_fine, 1.0)
```

```python
import functools

import jax
import jax.numpy as jnp
from jax import lax
from jax.experimental import pallas as pl
from jax.experimental.pallas import tpu as pltpu
from jax.sharding import PartitionSpec as P

BOX = 16
SEND = 2
W = 4
F32 = jnp.float32
MESH = pl.DeviceIdType.MESH
HIGH = lax.Precision.HIGHEST


def iota(shape, dim):
    return lax.broadcasted_iota(jnp.int32, shape, dim)


def up(v, axis):
    return pltpu.roll(v, 1, axis)


def down(v, axis):
    return pltpu.roll(v, v.shape[axis] - 1, axis)


class Level:
    def __init__(self, x, y, z):
        self.x, self.y, self.z = x, y, z
        self.xe, self.ye = x + 2 * W, y + 2 * W
        self.ze = 128 if z + 2 * W <= 128 else z + 128
        self.own = 128
        self.tiles = -(-self.xe // 16)
        self.shape = (self.xe, self.ye, self.ze)


def axis_info(axis, counts):
    me = lax.axis_index(axis)
    n = counts[axis]
    return me, n


def send_pair(axis, n, pairs, sends, recvs):
    me = lax.axis_index(axis)
    (low_src, low_dst), (high_src, high_dst) = pairs
    low = pltpu.make_async_remote_copy(
        low_src, low_dst, sends.at[0], recvs.at[0],
        device_id={axis: lax.rem(me + n - 1, n)}, device_id_type=MESH)
    high = pltpu.make_async_remote_copy(
        high_src, high_dst, sends.at[1], recvs.at[1],
        device_id={axis: lax.rem(me + 1, n)}, device_id_type=MESH)
    has_low, has_high = me > 0, me < n - 1

    @pl.when(has_low)
    def _():
        low.start()

    @pl.when(has_high)
    def _():
        high.start()

    def finish():
        @pl.when(has_low)
        def _():
            low.wait_send()
            high.wait_recv()

        @pl.when(has_high)
        def _():
            high.wait_send()
            low.wait_recv()

    return finish


def exchange(lv, v, bufs, counts):
    py, ly, pz, lz, sends, recvs = bufs
    own = (pl.ds(0, lv.y), pl.ds(0, lv.own))
    finish = send_pair(
        "gx", counts["gx"],
        ((v.at[(pl.ds(W, W),) + own], v.at[(pl.ds(lv.x + W, W),) + own]),
         (v.at[(pl.ds(lv.x, W),) + own], v.at[(pl.ds(0, W),) + own])),
        sends.at[0], recvs.at[0])
    yield
    finish()
    py[0] = v[:, 0:W, 0:lv.own]
    py[1] = v[:, lv.y - W : lv.y, 0:lv.own]
    finish = send_pair(
        "gy", counts["gy"], ((py.at[0], ly.at[0]), (py.at[1], ly.at[1])), sends.at[1], recvs.at[1])
    yield
    finish()
    v[:, lv.y : lv.y + W, 0:lv.own] = ly[0]
    v[:, lv.y + W : lv.ye, 0:lv.own] = ly[1]
    lane = iota((lv.ye, 128), 1)
    for tile in range(lv.tiles):
        packed = jnp.zeros((lv.ye, 128), F32)
        for k in range(min(16, lv.xe - 16 * tile)):
            plane = v[16 * tile + k, :, 0:128]
            if lv.z == 64:
                plane = jnp.where(lane >= 64, pltpu.roll(plane, 64, 1), plane)
            packed = jnp.where(lane // 8 == k, pltpu.roll(plane, (8 * k + W) % 128, 1), packed)
        pz[tile] = packed
    finish = send_pair("gz", counts["gz"], ((pz, lz.at[0]), (pz, lz.at[1])), sends.at[2], recvs.at[2])
    yield
    finish()
    edge = (lane < W) | (lane >= 128 - W)
    for tile in range(lv.tiles):
        both = jnp.where(lane % 8 >= W, lz[0, tile], lz[1, tile])
        for k in range(min(16, lv.xe - 16 * tile)):
            x = 16 * tile + k
            strip = jnp.where(edge, pltpu.roll(both, (256 - 8 * k - W) % 128, 1), 0.0)
            if lv.z == 64:
                v[x] = jnp.where(lane < 64, v[x], jnp.where(lane >= 128 - W, strip, pltpu.roll(strip, 64, 1)))
            else:
                v[x, :, lv.z : lv.z + 128] = strip
    yield


def gather(buf, sends, recvs, counts):
    at = {axis: lax.axis_index(axis) for axis in counts}
    prefix = {"gz": (at["gx"], at["gy"]), "gy": (at["gx"],), "gx": ()}
    base = 0
    for axis in ("gz", "gy", "gx"):
        me, n = at[axis], counts[axis]
        copies = []
        for k in range(1, n):
            block = buf.at[prefix[axis] + (me,)]
            copy = pltpu.make_async_remote_copy(
                block, block, sends.at[base + k - 1], recvs.at[base + k - 1],
                device_id={axis: lax.rem(me + k, n)}, device_id_type=MESH)
            copy.start()
            source = buf.at[prefix[axis] + (lax.rem(me + n - k, n),)]
            arrive = pltpu.make_async_remote_copy(
                source, source, sends.at[base + k - 1], recvs.at[base + k - 1],
                device_id={axis: lax.rem(me + k, n)}, device_id_type=MESH)
            copies.append((copy, arrive))
        yield
        for copy, arrive in copies:
            copy.wait_send()
            arrive.wait_recv()
        base += n - 1
    yield


def together(*steps):
    for _ in zip(*steps):
        pass


def prepare(lv, k, fx, fy, fz, dd, iv):
    def body(x, carry):
        kx = k[x]
        below = 0.5 * (k[jnp.maximum(x - 1, 0)] + kx)
        above = 0.5 * (kx + k[jnp.minimum(x + 1, lv.xe - 1)])
        second = 0.5 * (up(kx, 0) + kx)
        third = 0.5 * (up(kx, 1) + kx)
        total = below + above + second + down(second, 0) + third + down(third, 1)
        fx[x], fy[x], fz[x], dd[x] = below, second, third, total
        iv[x] = jnp.where(kx > 0.0, 1.0 / total, 0.0)
        return carry

    lax.fori_loop(0, lv.xe, body, 0)


def around(v, x, mid, faces):
    fx, fy, fz = faces
    second, third = fy[x], fz[x]
    summed = fx[x] * v[x - 1] + fx[x + 1] * v[x + 1]
    summed = summed + second * up(mid, 0) + down(second * mid, 0)
    return summed + third * up(mid, 1) + down(third * mid, 1)


def half_sweep(lv, v, g, faces, iv, colour, batch):
    parity = iota((lv.ye, lv.ze), 0) + iota((lv.ye, lv.ze), 1)

    def body(step, carry):
        fresh = []
        for k in range(batch):
            x = 1 + step * batch + k
            mid = v[x]
            value = (g[x] + around(v, x, mid, faces)) * iv[x]
            fresh.append((x, jnp.where((parity + x) % 2 == colour, value, mid)))
        for x, value in fresh:
            v[x] = value
        return carry

    lax.fori_loop(0, (lv.xe - 2) // batch, body, 0)


def residual_pairs(lv, v, g, faces, dd, pairs):
    def body(i, carry):
        total = jnp.zeros((lv.ye, lv.ze), F32)
        for k in range(2):
            x = W + 2 * i + k
            mid = v[x]
            total = total + (g[x] - dd[x] * mid + around(v, x, mid, faces))
        pairs[i] = total[0 : lv.y, 0 : lv.own]
        return carry

    lax.fori_loop(0, lv.x // 2, body, 0)


def open_halo(lv, p, v, g, dd):
    parity = iota((lv.ye, lv.ze), 0) + iota((lv.ye, lv.ze), 1)

    def body(x, carry):
        red = (parity + x) % 2 == 0
        px = p[x]
        v[x] = jnp.where(red, px, 0.0)
        g[x] = jnp.where(red, px * dd[x], px)
        return carry

    lax.fori_loop(0, lv.xe, body, 0)


def fold_rows(pairs, rows):
    return pairs[:, pl.ds(0, rows, stride=2), :] + pairs[:, pl.ds(1, rows, stride=2), :]


def dot(a, b):
    return jnp.dot(a, b, precision=HIGH, preferred_element_type=F32)


def coarse_mid(pairs, x, y):
    folded = fold_rows(pairs, y // 2).reshape((x // 2) * (y // 2), 128)
    matrix = jnp.where(iota((128, 128), 0) // 2 == iota((128, 128), 1), 0.125, 0.0).astype(F32)
    return dot(folded, matrix).reshape(x // 2, y // 2, 128)


def coarse_low(pairs, count, rows, lanes, tmp, target):
    total = jnp.zeros((rows, 128), F32)
    source, goal = iota((128, 128), 0), iota((128, 128), 1)
    for x in range(count):
        matrix = jnp.where((source // 2 + x * lanes == goal) & (source < 2 * lanes), 0.125, 0.0).astype(F32)
        total = total + dot(pairs[x], matrix)
    tmp[...] = total
    half = rows // 2
    small = tmp[pl.ds(0, half, stride=2), :] + tmp[pl.ds(1, half, stride=2), :]
    target[0:half, :] = small
    target[half:rows, :] = small


def spread_low(buf, whole, counts, pad):
    lane, row = iota((8, 128), 1), iota((8, 128), 0)

    def body(a, carry):
        for i in range(4):
            for ct in range(counts["gy"] // 2):
                for gt in range(counts["gz"] // 4):
                    total = jnp.zeros((8, 128), F32)
                    for c in range(2):
                        for g in range(4):
                            piece = pltpu.roll(buf[a, 2 * ct + c, 4 * gt + g], (32 * (g - i)) % 128, 1)
                            total = jnp.where((lane // 32 == g) & (row // 4 == c), piece, total)
                    whole[pad + 4 * a + i, 8 * ct : 8 * ct + 8, 128 * gt : 128 * gt + 128] = total
        return carry

    lax.fori_loop(0, counts["gx"], body, 0)


def bottom(f, k, s, vv, xs, dims):
    planes, rows, lanes = dims
    row, lane = iota((rows, lanes), 0), iota((rows, lanes), 1)
    edges = (row > 0, row < rows - 1, lane > 0, lane < lanes - 1)

    def shifted(v):
        return (
            jnp.where(edges[0], up(v, 0), 0.0), jnp.where(edges[1], down(v, 0), 0.0),
            jnp.where(edges[2], up(v, 1), 0.0), jnp.where(edges[3], down(v, 1), 0.0))

    def operate(v, x):
        kx, mid = k[x], v[x]
        summed, diagonal = jnp.zeros_like(mid), jnp.zeros_like(mid)
        others = ((k[x - 1], v[x - 1]), (k[x + 1], v[x + 1])) + tuple(zip(shifted(kx), shifted(mid)))
        for other, value in others:
            face = 0.5 * (kx + other)
            diagonal = diagonal + face
            summed = summed + face * value
        return mid, (diagonal * mid - summed) * 0.0625

    zero = jnp.zeros((rows, lanes), F32)

    def first(x, carry):
        mid, image = operate(f, x + 1)
        vv[x] = image
        return carry[0] + mid * mid, carry[1] + mid * image

    def total(v):
        return jnp.sum(jnp.sum(v, axis=0, keepdims=True), axis=1, keepdims=True)

    norm, along = lax.fori_loop(0, planes, first, (zero, zero))
    alpha = total(norm) / total(along)

    def rest(x, carry):
        s[x + 1] = f[x + 1] - alpha * vv[x]
        return carry

    lax.fori_loop(0, planes, rest, 0)

    def second(x, carry):
        mid, image = operate(s, x + 1)
        return carry[0] + image * mid, carry[1] + image * image

    turned, norm = lax.fori_loop(0, planes, second, (zero, zero))
    omega = total(turned) / total(norm)

    def join(x, carry):
        xs[x + 2] = alpha * f[x + 1] + omega * s[x + 1]
        return carry

    lax.fori_loop(0, planes, join, 0)


def pack_boxes(slots, ids, outgoing, boxes, groups):
    held = ids[0].astype(F32)
    cap = held.shape[1]
    eye = iota((cap, cap), 0) == iota((cap, cap), 1)
    rows = jnp.broadcast_to(held, (cap, cap))
    cols = jnp.broadcast_to(jnp.sum(jnp.where(eye, rows, 0.0), axis=1, keepdims=True), (cap, cap))

    def target(v):
        return jnp.floor((v + 0.5) * (1.0 / boxes))

    earlier = (target(rows) == target(cols)) & (cols < rows) & (cols >= 0.0)
    ranking = jnp.sum(jnp.where(earlier, 1.0, 0.0), axis=0, keepdims=True)
    send_row = jnp.where(held >= 0.0, target(held) * SEND + ranking, -1.0)
    count = groups * SEND
    picker = jnp.where(iota((count, cap), 0).astype(F32) == jnp.broadcast_to(send_row, (count, cap)), 1.0, 0.0)
    data = slots[0, 0].astype(F32)
    total = jnp.zeros((count, data.shape[1]), F32)
    for q in range(cap):
        total = total + picker[:, q : q + 1] * data[q : q + 1, :]
    for t in range(groups):
        outgoing[t] = total[SEND * t : SEND * t + SEND, :]


def place_boxes(incoming, owner, lhs, rhs, boxes, groups):
    me = lax.axis_index("gz")
    owners = jnp.broadcast_to(owner[0].astype(F32), (boxes, owner.shape[2]))
    here = iota(owners.shape, 1) == iota(owners.shape, 0) + me * boxes
    col = jnp.sum(jnp.where(here, owners, 0.0), axis=1, keepdims=True)
    cols = jnp.broadcast_to(col, (boxes, boxes))
    first, second = iota((boxes, boxes), 0), iota((boxes, boxes), 1)
    row = jnp.sum(jnp.where(first == second, cols, 0.0), axis=0, keepdims=True)
    before = (jnp.broadcast_to(row, (boxes, boxes)) == cols) & (second < first)
    pick = col * SEND + jnp.sum(jnp.where(before, 1.0, 0.0), axis=1, keepdims=True)
    face = BOX * BOX
    mine = iota((BOX, face), 1) // BOX == iota((BOX, face), 0)
    for i in range(BOX):
        chosen = jnp.zeros((boxes, face), F32)
        for r in range(groups * SEND):
            chosen = jnp.where(pick == float(r), incoming[r // SEND, r % SEND : r % SEND + 1, face * i : face * i + face], chosen)
        for b in range(boxes):
            piece = jnp.where(mine, jnp.broadcast_to(chosen[b : b + 1, :], (BOX, face)), 0.0)
            lhs[BOX * i : BOX * i + BOX, face * b : face * b + face] = piece.astype(jnp.bfloat16)
    return jnp.dot(lhs[...], rhs[...], preferred_element_type=F32)


def kernel(fine, mid, counts, names, slots, ids, owner, coef, out, *scratch):
    r = dict(zip(names, scratch))
    groups = counts["gz"]
    boxes = fine.z // BOX
    at = {axis: lax.axis_index(axis) for axis in counts}
    for name in ("K0", "P0", "Q0", "K1", "P1", "E1", "ly", "lz", "lym", "lzm", "f2", "k2", "s2", "x2"):
        r[name][...] = jnp.zeros(r[name].shape, F32)

    barrier = pltpu.get_barrier_semaphore()
    for axis, n in counts.items():
        for k in range(1, n):
            pl.semaphore_signal(
                barrier, inc=1, device_id={axis: lax.rem(at[axis] + k, n)}, device_id_type=MESH)

    pack_boxes(slots, ids, r["outgoing"], boxes, groups)
    K0, K1 = r["K0"], r["K1"]
    K0[W : W + fine.x, 0 : fine.y, 0:128] = coef[...]
    for i in range(mid.x):
        r["pairs"][i] = coef[2 * i] + coef[2 * i + 1]
    K1[W : W + mid.x, 0 : mid.y, :] = coarse_mid(r["pairs"], fine.x, fine.y)
    for i in range(mid.x // 2):
        r["pairsm"][i] = K1[W + 2 * i, 0 : mid.y, :] + K1[W + 2 * i + 1, 0 : mid.y, :]
    here = (at["gx"], at["gy"], at["gz"])
    coarse_low(r["pairsm"], mid.x // 2, mid.y, mid.z // 2, r["tmp"], r["gk"].at[here])
    pl.semaphore_wait(barrier, sum(counts.values()) - len(counts))

    moves = []
    me = at["gz"]
    for k in range(1, groups):
        to, source = lax.rem(me + k, groups), lax.rem(me + groups - k, groups)
        copy = pltpu.make_async_remote_copy(
            r["outgoing"].at[to], r["incoming"].at[me], r["ms"].at[k - 1], r["mr"].at[k - 1],
            device_id={"gz": to}, device_id_type=MESH)
        copy.start()
        arrive = pltpu.make_async_remote_copy(
            r["outgoing"].at[to], r["incoming"].at[source], r["ms"].at[k - 1], r["mr"].at[k - 1],
            device_id={"gz": to}, device_id_type=MESH)
        moves.append((copy, arrive))
    r["incoming"][me] = r["outgoing"][me]

    def bufs(n, tail):
        return tuple(r[b + tail].at[n] for b in ("py", "ly", "pz", "lz", "es", "er"))

    steps = [
        exchange(fine, K0, bufs(0, ""), counts), exchange(mid, K1, bufs(0, "m"), counts),
        gather(r["gk"], r["gs"].at[0], r["gr"].at[0], counts)]
    for step in steps:
        next(step)
    lane = iota((BOX * BOX, 128), 1)
    folded = iota((BOX * BOX, 128), 0) % BOX == lane % BOX
    for b in range(boxes):
        block = jnp.where(folded & (lane // BOX == b), 1.0, 0.0)
        r["rhs"][BOX * BOX * b : BOX * BOX * (b + 1), :] = block.astype(jnp.bfloat16)
    for copy, arrive in moves:
        copy.wait_send()
        arrive.wait_recv()
    source = place_boxes(r["incoming"], owner, r["lhs"], r["rhs"], boxes, groups)
    source = source.reshape(fine.x, fine.y, 128)
    together(*steps)

    faces0 = (r["fx0"], r["fy0"], r["fz0"])
    faces1 = (r["fx1"], r["fy1"], r["fz1"])
    dd0, iv0, dd1, iv1 = r["dd0"], r["iv0"], r["dd1"], r["iv1"]
    v0, g0, v1, g1 = r["v0"], r["g0"], r["v1"], r["g1"]
    prepare(fine, K0, *faces0, dd0, iv0)
    parity = iota((fine.y, 128), 0) + iota((fine.y, 128), 1)
    for x in range(fine.x):
        red = (parity + x) % 2 == 0
        r["P0"][W + x, 0 : fine.y, 0:128] = jnp.where(red, source[x] * iv0[W + x, 0 : fine.y, 0:128], source[x])
    step = exchange(fine, r["P0"], bufs(1, ""), counts)
    next(step)
    prepare(mid, K1, *faces1, dd1, iv1)
    together(step)
    open_halo(fine, r["P0"], v0, g0, dd0)
    for colour in (1, 0, 1):
        half_sweep(fine, v0, g0, faces0, iv0, colour, 2)
    residual_pairs(fine, v0, g0, faces0, dd0, r["pairs"])

    source1 = coarse_mid(r["pairs"], fine.x, fine.y)
    parity = iota((mid.y, 128), 0) + iota((mid.y, 128), 1)
    for x in range(mid.x):
        red = (parity + x) % 2 == 0
        scaled = 4.0 * source1[x]
        r["P1"][W + x, 0 : mid.y, :] = jnp.where(red, scaled * iv1[W + x, 0 : mid.y, :], scaled)
    step = exchange(mid, r["P1"], bufs(1, "m"), counts)
    next(step)
    spread_low(r["gk"], r["k2"], counts, 1)
    together(step)
    open_halo(mid, r["P1"], v1, g1, dd1)
    for colour in (1, 0, 1):
        half_sweep(mid, v1, g1, faces1, iv1, colour, 2)
    residual_pairs(mid, v1, g1, faces1, dd1, r["pairsm"])
    for i in range(mid.x // 2):
        r["pairsm"][i] = r["pairsm"][i] * 0.25
    coarse_low(r["pairsm"], mid.x // 2, mid.y, mid.z // 2, r["tmp"], r["gf"].at[here])
    r["E1"][W : W + mid.x, 0 : mid.y, :] = v1[W : W + mid.x, 0 : mid.y, :]
    together(
        gather(r["gf"], r["gs"].at[1], r["gr"].at[1], counts),
        exchange(mid, r["E1"], bufs(2, "m"), counts))

    planes, rows, lanes = 4 * counts["gx"], 4 * counts["gy"], 32 * counts["gz"]
    spread_low(r["gf"], r["f2"], counts, 1)
    bottom(r["f2"], r["k2"], r["s2"], r["v2"], r["x2"], (planes, rows, lanes))
    row8 = iota((8, lanes), 0)
    for q in range(8):
        plane = r["x2"][4 * at["gx"] + q]
        turned = plane
        for c in range(1, counts["gy"]):
            turned = jnp.where(at["gy"] == c, pltpu.roll(plane, rows - 4 * c, 0), turned)
        r["local"][q] = jnp.where(row8 < 6, turned[0:8, :], turned[rows - 8 : rows, :])
    goal = iota((lanes, 128), 1)
    cell = jnp.where(goal < mid.z + W, goal, goal - 128)
    cell = (cell + 128) // 2 - 64
    wanted = (goal < mid.z + W) | (goal >= 128 - W)
    matrix = jnp.where((iota((lanes, 128), 0) == 32 * at["gz"] + cell) & wanted, 1.0, 0.0).astype(F32)
    spread = dot(r["local"][...].reshape(64, lanes), matrix).reshape(8, 8, 128)
    E1 = r["E1"]
    for q in range(8):
        r["wide"][pl.ds(0, 8, stride=2), :] = spread[q]
        r["wide"][pl.ds(1, 8, stride=2), :] = spread[q]
        for k in range(2):
            x = 2 * q + k
            E1[x] = jnp.where(K1[x] > 0.0, E1[x] + r["wide"][...], 0.0)
    for colour in (0, 1, 0, 1):
        half_sweep(mid, E1, g1, faces1, iv1, colour, 2)

    matrix = jnp.where(iota((128, 128), 0) == iota((128, 128), 1) // 2, 1.0, 0.0).astype(F32)
    fresh = dot(E1[W : W + mid.x, 0 : mid.y, :].reshape(mid.x * mid.y, 128), matrix).reshape(mid.x, mid.y, 128)
    Q0 = r["Q0"]
    for i in range(mid.x):
        r["wide"][pl.ds(0, mid.y, stride=2), :] = fresh[i]
        r["wide"][pl.ds(1, mid.y, stride=2), :] = fresh[i]
        for k in range(2):
            x = W + 2 * i + k
            Q0[x, 0 : fine.y, 0:128] = v0[x, 0 : fine.y, 0:128] + r["wide"][...]
    together(exchange(fine, Q0, bufs(2, ""), counts))
    for colour in (0, 1, 0, 1):
        half_sweep(fine, Q0, g0, faces0, iv0, colour, 2)
    out[...] = Q0[W : W + fine.x, 0 : fine.y, 0:128]


def per_device(counts, old_slots, old_ids, old_owner, coefficient):
    x, y, z = coefficient.shape
    fine, mid = Level(x, y, z), Level(x // 2, y // 2, z // 2)
    planes, rows, lanes = 4 * counts["gx"], 4 * counts["gy"], 32 * counts["gz"]
    groups, boxes = counts["gz"], z // BOX
    cells = old_slots.shape[3]
    partners = sum(counts.values()) - len(counts)
    vmem = lambda *shape: pltpu.VMEM(shape, F32)
    dma = lambda *shape: pltpu.SemaphoreType.DMA(shape)
    scratch = {}
    for level, tail, names in ((fine, "", ("K0", "P0", "Q0")), (mid, "m", ("K1", "P1", "E1"))):
        for name in names:
            scratch[name] = vmem(*level.shape)
        scratch["py" + tail] = vmem(3, 2, level.xe, W, 128)
        scratch["ly" + tail] = vmem(3, 2, level.xe, W, 128)
        scratch["pz" + tail] = vmem(3, level.tiles, level.ye, 128)
        scratch["lz" + tail] = vmem(3, 2, level.tiles, level.ye, 128)
        scratch["es" + tail] = dma(3, 3, 2)
        scratch["er" + tail] = dma(3, 3, 2)
        scratch["pairs" + tail] = vmem(level.x // 2, level.y, 128)
    for level, tail in ((fine, "0"), (mid, "1")):
        for name in ("fx", "fy", "fz", "dd", "iv", "v", "g"):
            scratch[name + tail] = vmem(*level.shape)
    scratch.update(
        outgoing=vmem(groups, SEND, cells), incoming=vmem(groups, SEND, cells), ms=dma(groups - 1), mr=dma(groups - 1),
        lhs=pltpu.VMEM((BOX * BOX, boxes * BOX * BOX), jnp.bfloat16),
        rhs=pltpu.VMEM((boxes * BOX * BOX, 128), jnp.bfloat16),
        tmp=vmem(mid.y, 128), wide=vmem(16, 128), local=vmem(8, 8, lanes),
        gk=vmem(counts["gx"], counts["gy"], groups, 8, 128), gf=vmem(counts["gx"], counts["gy"], groups, 8, 128),
        gs=dma(2, partners), gr=dma(2, partners),
        f2=vmem(planes + 2, rows, lanes), k2=vmem(planes + 2, rows, lanes), s2=vmem(planes + 2, rows, lanes),
        v2=vmem(planes, rows, lanes), x2=vmem(planes + 4, rows, lanes))
    return pl.pallas_call(
        functools.partial(kernel, fine, mid, counts, tuple(scratch)),
        out_shape=jax.ShapeDtypeStruct(coefficient.shape, F32),
        in_specs=[pl.BlockSpec(memory_space=pltpu.VMEM)] * 4,
        out_specs=pl.BlockSpec(memory_space=pltpu.VMEM),
        scratch_shapes=list(scratch.values()),
        compiler_params=pltpu.CompilerParams(
            collective_id=0, has_side_effects=True, vmem_limit_bytes=60 * 1024 * 1024),
    )(old_slots, old_ids, old_owner, coefficient)


def solution(mesh):
    counts = {axis: mesh.shape[axis] for axis in ("gx", "gy", "gz")}
    return jax.shard_map(
        functools.partial(per_device, counts), mesh=mesh,
        in_specs=(P("gx", "gy", "gz", None), P("gx", "gy", "gz"), P("gx", "gy", None), P("gx", "gy", "gz")),
        out_specs=P("gx", "gy", "gz"), check_vma=False)
```

```python
import functools

import jax
import jax.numpy as jnp
from jax import lax
from jax.experimental import pallas as pl
from jax.experimental.pallas import tpu as pltpu
from jax.sharding import PartitionSpec as P

BOX = 16
SEND = 2
W = 4
F32 = jnp.float32
MESH = pl.DeviceIdType.MESH
HIGH = lax.Precision.HIGHEST


def iota(shape, dim):
    return lax.broadcasted_iota(jnp.int32, shape, dim)


def up(v, axis):
    return pltpu.roll(v, 1, axis)


def down(v, axis):
    return pltpu.roll(v, v.shape[axis] - 1, axis)


class Level:
    def __init__(self, x, y, z):
        self.x, self.y, self.z = x, y, z
        self.xe, self.ye = x + 2 * W, y + 2 * W
        self.ze = 128 if z + 2 * W <= 128 else z + 128
        self.shape = (self.xe, self.ye, self.ze)


NEAR = [(a, b, c) for c in (-1, 0, 1) for b in (-1, 0, 1) for a in (-1, 0, 1) if (a, b, c) != (0, 0, 0)]


def near(offset, counts):
    target, exists = {}, None
    for axis, step in zip(("gx", "gy", "gz"), offset):
        me, n = lax.axis_index(axis), counts[axis]
        if step:
            target[axis] = lax.rem(me + step + n, n)
            inside = me > 0 if step < 0 else me < n - 1
            exists = inside if exists is None else jnp.logical_and(exists, inside)
    return target, exists


def exchange(lv, v, bufs, counts):
    py, ly, pz, lz, sends, recvs = bufs
    own = slice(W, W + lv.x)
    py[0] = v[own, 0:W, 0:128]
    py[1] = v[own, lv.y - W : lv.y, 0:128]
    lane = iota((lv.y, 128), 1)
    packed = jnp.zeros((lv.y, 128), F32)
    for k in range(lv.x):
        plane = v[W + k, 0 : lv.y, 0:128]
        if lv.z == 64:
            plane = jnp.where(lane >= 64, pltpu.roll(plane, 64, 1), plane)
        packed = jnp.where(lane // 8 == k, pltpu.roll(plane, (8 * k + W) % 128, 1), packed)
    pz[...] = packed
    block = (pl.ds(0, lv.y), pl.ds(0, 128))
    taken = {-1: (0, W), 0: (0, lv.x), 1: (lv.x - W, W)}
    landed = {-1: lv.x + W, 0: W, 1: 0}
    copies = []
    for at, (a, b, c) in enumerate(NEAR):
        target, exists = near((a, b, c), counts)
        first, count = taken[a]
        if c:
            src, dst = pz, lz.at[(1 - c) // 2, 1 - a, 1 - b]
        elif b:
            side = (b + 1) // 2
            src, dst = py.at[side, pl.ds(first, count)], ly.at[side, pl.ds(landed[a], count)]
        else:
            src, dst = v.at[(pl.ds(W + first, count),) + block], v.at[(pl.ds(landed[a], count),) + block]
        copy = pltpu.make_async_remote_copy(
            src, dst, sends.at[at], recvs.at[at], device_id=target, device_id_type=MESH)
        copies.append(((a, b, c), copy, exists))
    for _, copy, exists in reversed(copies):
        pl.when(exists)(copy.start)
    yield
    for (a, b, c), copy, exists in copies:
        pl.when(exists)(copy.wait_send)
        pl.when(near((-a, -b, -c), counts)[1])(copy.wait_recv)
    v[:, lv.y : lv.y + W, 0:128] = ly[0]
    v[:, lv.y + W : lv.ye, 0:128] = ly[1]
    row = iota((8, 128), 0)
    side = iota((lv.ye, 128), 1)
    edge = (side < W) | (side >= 128 - W)
    for a in range(3):
        parts = []
        for c in range(2):
            ends = jnp.where(row < W, lz[c, a, 2, 0:8, :], lz[c, a, 0, lv.y - 8 : lv.y, :])
            parts.append(jnp.concatenate([lz[c, a, 1], ends], axis=0))
        both = jnp.where(side % 8 >= W, parts[1], parts[0])
        first = (0, W, lv.x + W)[a]
        start, count = ((lv.x - W, W), (0, lv.x), (0, W))[a]
        for k in range(count):
            x = first + k
            strip = jnp.where(edge, pltpu.roll(both, (256 - 8 * (start + k) - W) % 128, 1), 0.0)
            if lv.z == 64:
                v[x] = jnp.where(side < 64, v[x], jnp.where(side >= 128 - W, strip, pltpu.roll(strip, 64, 1)))
            else:
                v[x, :, lv.z : lv.z + 128] = strip
    yield


def gather(buf, sends, recvs, counts):
    me = {axis: lax.axis_index(axis) for axis in counts}
    nx, ny, nz = counts["gx"], counts["gy"], counts["gz"]

    def run(steps, base):
        copies = []
        for at, (target, mine, theirs) in enumerate(steps):
            pair = (sends.at[base + at], recvs.at[base + at])
            copy = pltpu.make_async_remote_copy(mine, mine, *pair, device_id=target, device_id_type=MESH)
            copy.start()
            copies.append((copy, pltpu.make_async_remote_copy(
                theirs, theirs, *pair, device_id=target, device_id_type=MESH)))
        yield
        for copy, arrive in copies:
            copy.wait_send()
            arrive.wait_recv()

    steps = []
    for b in range(ny):
        for c in range(nz):
            if b or c:
                target = {"gy": lax.rem(me["gy"] + b, ny), "gz": lax.rem(me["gz"] + c, nz)}
                source = buf.at[me["gx"], lax.rem(me["gy"] + ny - b, ny), lax.rem(me["gz"] + nz - c, nz)]
                steps.append((target, buf.at[me["gx"], me["gy"], me["gz"]], source))
    yield from run(steps, 0)
    base = len(steps)
    steps = [({"gx": lax.rem(me["gx"] + a, nx)}, buf.at[me["gx"]], buf.at[lax.rem(me["gx"] + nx - a, nx)]) for a in range(1, nx)]
    yield from run(steps, base)


def drain(*steps):
    steps = list(steps)
    while steps:
        steps = [step for step in steps if next(step, steps) is not steps]


def batches(low, high, size, body):
    whole = (high - low) // size
    if whole:
        def run(step, carry):
            body(low + step * size, size)
            return carry

        lax.fori_loop(0, whole, run, 0)
    if low + whole * size < high:
        body(low + whole * size, high - low - whole * size)


def prepare(lv, k, fx, fy, fz, dd, iv):
    def body(first, count):
        made = []
        for x in [first + i for i in range(count)]:
            kx = k[x]
            below = 0.5 * (k[jnp.maximum(x - 1, 0)] + kx)
            above = 0.5 * (kx + k[jnp.minimum(x + 1, lv.xe - 1)])
            second = 0.5 * (up(kx, 0) + kx)
            third = 0.5 * (up(kx, 1) + kx)
            total = below + above + second + down(second, 0) + third + down(third, 1)
            made.append((x, below, second, third, total, jnp.where(kx > 0.0, 1.0 / total, 0.0)))
        for x, *values in made:
            for ref, value in zip((fx, fy, fz, dd, iv), values):
                ref[x] = value

    batches(0, lv.xe, 4 if lv.ze == 128 else 2, body)


def around(v, x, mid, faces):
    fx, fy, fz = faces
    second, third = fy[x], fz[x]
    summed = fx[x] * v[x - 1] + fx[x + 1] * v[x + 1]
    summed = summed + second * up(mid, 0) + down(second * mid, 0)
    return summed + third * up(mid, 1) + down(third * mid, 1)


def half_sweep(lv, v, g, faces, iv, colour, reach):
    parity = iota((lv.ye, lv.ze), 0) + iota((lv.ye, lv.ze), 1)

    def body(first, count):
        fresh = []
        for x in [first + i for i in range(count)]:
            mid = v[x]
            value = (g[x] + around(v, x, mid, faces)) * iv[x]
            fresh.append((x, jnp.where(((parity + x) & 1) == colour, value, mid)))
        for x, value in fresh:
            v[x] = value

    batches(W - reach, W + lv.x + reach, 10 if lv.ze == 128 else 6, body)


def residual_pairs(lv, v, g, faces, dd, pairs):
    def body(first, count):
        made = []
        for i in [first + j for j in range(count)]:
            total = jnp.zeros((lv.ye, lv.ze), F32)
            for k in range(2):
                x = W + 2 * i + k
                mid = v[x]
                total = total + (g[x] - dd[x] * mid + around(v, x, mid, faces))
            made.append((i, total))
        for i, total in made:
            pairs[i] = total[0 : lv.y, 0:128]

    batches(0, lv.x // 2, 4, body)


def open_halo(lv, p, v, g, dd):
    parity = iota((lv.ye, lv.ze), 0) + iota((lv.ye, lv.ze), 1)

    def body(first, count):
        made = []
        for x in [first + i for i in range(count)]:
            red = ((parity + x) & 1) == 0
            px = p[x]
            made.append((x, jnp.where(red, px, 0.0), jnp.where(red, px * dd[x], px)))
        for x, value, source in made:
            v[x] = value
            g[x] = source

    batches(0, lv.xe, 4, body)


def fold_rows(pairs, rows):
    return pairs[:, pl.ds(0, rows, stride=2), :] + pairs[:, pl.ds(1, rows, stride=2), :]


def dot(a, b):
    return jnp.dot(a, b, precision=HIGH, preferred_element_type=F32)


def coarse_mid(pairs, x, y):
    folded = fold_rows(pairs, y // 2).reshape((x // 2) * (y // 2), 128)
    matrix = jnp.where(iota((128, 128), 0) // 2 == iota((128, 128), 1), 0.125, 0.0).astype(F32)
    return dot(folded, matrix).reshape(x // 2, y // 2, 128)


def coarse_low(pairs, count, rows, lanes, tmp, target):
    total = jnp.zeros((rows, 128), F32)
    source, goal = iota((128, 128), 0), iota((128, 128), 1)
    for x in range(count):
        matrix = jnp.where((source // 2 + x * lanes == goal) & (source < 2 * lanes), 0.125, 0.0).astype(F32)
        total = total + dot(pairs[x], matrix)
    tmp[...] = total
    half = rows // 2
    small = tmp[pl.ds(0, half, stride=2), :] + tmp[pl.ds(1, half, stride=2), :]
    target[0:half, :] = small
    target[half:rows, :] = small


def spread_low(buf, whole, counts, pad):
    lane, row = iota((8, 128), 1), iota((8, 128), 0)

    def body(a, carry):
        for i in range(4):
            for ct in range(counts["gy"] // 2):
                for gt in range(counts["gz"] // 4):
                    total = jnp.zeros((8, 128), F32)
                    for c in range(2):
                        for g in range(4):
                            piece = pltpu.roll(buf[a, 2 * ct + c, 4 * gt + g], (32 * (g - i)) % 128, 1)
                            total = jnp.where((lane // 32 == g) & (row // 4 == c), piece, total)
                    whole[pad + 4 * a + i, 8 * ct : 8 * ct + 8, 128 * gt : 128 * gt + 128] = total
        return carry

    lax.fori_loop(0, counts["gx"], body, 0)


def bottom(f, k, s, vv, xs, dims):
    planes, rows, lanes = dims
    row, lane = iota((rows, lanes), 0), iota((rows, lanes), 1)
    edges = (row > 0, row < rows - 1, lane > 0, lane < lanes - 1)

    def shifted(v):
        return (
            jnp.where(edges[0], up(v, 0), 0.0), jnp.where(edges[1], down(v, 0), 0.0),
            jnp.where(edges[2], up(v, 1), 0.0), jnp.where(edges[3], down(v, 1), 0.0))

    def operate(v, x):
        kx, mid = k[x], v[x]
        summed, diagonal = jnp.zeros_like(mid), jnp.zeros_like(mid)
        others = ((k[x - 1], v[x - 1]), (k[x + 1], v[x + 1])) + tuple(zip(shifted(kx), shifted(mid)))
        for other, value in others:
            face = 0.5 * (kx + other)
            diagonal = diagonal + face
            summed = summed + face * value
        return mid, (diagonal * mid - summed) * 0.0625

    zero = jnp.zeros((rows, lanes), F32)

    def first(x, carry):
        mid, image = operate(f, x + 1)
        vv[x] = image
        return carry[0] + mid * mid, carry[1] + mid * image

    def total(v):
        return jnp.sum(jnp.sum(v, axis=0, keepdims=True), axis=1, keepdims=True)

    norm, along = lax.fori_loop(0, planes, first, (zero, zero))
    alpha = total(norm) / total(along)

    def rest(x, carry):
        s[x + 1] = f[x + 1] - alpha * vv[x]
        return carry

    lax.fori_loop(0, planes, rest, 0)

    def second(x, carry):
        mid, image = operate(s, x + 1)
        return carry[0] + image * mid, carry[1] + image * image

    turned, norm = lax.fori_loop(0, planes, second, (zero, zero))
    omega = total(turned) / total(norm)

    def join(x, carry):
        xs[x + 2] = alpha * f[x + 1] + omega * s[x + 1]
        return carry

    lax.fori_loop(0, planes, join, 0)


def pack_boxes(slots, ids, outgoing, boxes, groups):
    held = ids[0].astype(F32)
    cap = held.shape[1]
    eye = iota((cap, cap), 0) == iota((cap, cap), 1)
    rows = jnp.broadcast_to(held, (cap, cap))
    cols = jnp.broadcast_to(jnp.sum(jnp.where(eye, rows, 0.0), axis=1, keepdims=True), (cap, cap))

    def target(v):
        return jnp.floor((v + 0.5) * (1.0 / boxes))

    earlier = (target(rows) == target(cols)) & (cols < rows) & (cols >= 0.0)
    ranking = jnp.sum(jnp.where(earlier, 1.0, 0.0), axis=0, keepdims=True)
    send_row = jnp.where(held >= 0.0, target(held) * SEND + ranking, -1.0)
    count = groups * SEND
    picker = jnp.where(iota((count, cap), 0).astype(F32) == jnp.broadcast_to(send_row, (count, cap)), 1.0, 0.0)
    data = slots[0, 0].astype(F32)
    total = jnp.zeros((count, data.shape[1]), F32)
    for q in range(cap):
        total = total + picker[:, q : q + 1] * data[q : q + 1, :]
    for t in range(groups):
        outgoing[t] = total[SEND * t : SEND * t + SEND, :]


def place_boxes(incoming, owner, lhs, rhs, boxes, groups):
    me = lax.axis_index("gz")
    owners = jnp.broadcast_to(owner[0].astype(F32), (boxes, owner.shape[2]))
    here = iota(owners.shape, 1) == iota(owners.shape, 0) + me * boxes
    col = jnp.sum(jnp.where(here, owners, 0.0), axis=1, keepdims=True)
    cols = jnp.broadcast_to(col, (boxes, boxes))
    first, second = iota((boxes, boxes), 0), iota((boxes, boxes), 1)
    row = jnp.sum(jnp.where(first == second, cols, 0.0), axis=0, keepdims=True)
    before = (jnp.broadcast_to(row, (boxes, boxes)) == cols) & (second < first)
    pick = col * SEND + jnp.sum(jnp.where(before, 1.0, 0.0), axis=1, keepdims=True)
    face = BOX * BOX
    mine = iota((BOX, face), 1) // BOX == iota((BOX, face), 0)
    for i in range(BOX):
        chosen = jnp.zeros((boxes, face), F32)
        for r in range(groups * SEND):
            chosen = jnp.where(pick == float(r), incoming[r // SEND, r % SEND : r % SEND + 1, face * i : face * i + face], chosen)
        for b in range(boxes):
            piece = jnp.where(mine, jnp.broadcast_to(chosen[b : b + 1, :], (BOX, face)), 0.0)
            lhs[BOX * i : BOX * i + BOX, face * b : face * b + face] = piece.astype(jnp.bfloat16)
    return jnp.dot(lhs[...], rhs[...], preferred_element_type=F32)


def kernel(fine, mid, counts, names, slots, ids, owner, coef, out, *scratch):
    r = dict(zip(names, scratch))
    groups = counts["gz"]
    boxes = fine.z // BOX
    at = {axis: lax.axis_index(axis) for axis in counts}
    for name in ("K0", "P0", "Q0", "K1", "P1", "E1", "ly", "lz", "lym", "lzm", "f2", "k2", "s2", "x2"):
        r[name][...] = jnp.zeros(r[name].shape, F32)

    barrier = pltpu.get_barrier_semaphore()
    expected = 0
    for offset in NEAR:
        target, exists = near(offset, counts)

        @pl.when(exists)
        def _():
            pl.semaphore_signal(barrier, inc=1, device_id=target, device_id_type=MESH)

        expected = expected + jnp.where(exists, 1, 0)
    others = [{"gx": lax.rem(at["gx"] + k, counts["gx"])} for k in range(1, counts["gx"])]
    for b in range(counts["gy"]):
        for c in range(groups):
            if b or c:
                others.append({"gy": lax.rem(at["gy"] + b, counts["gy"]), "gz": lax.rem(at["gz"] + c, groups)})
    for target in others:
        pl.semaphore_signal(barrier, inc=1, device_id=target, device_id_type=MESH)

    pack_boxes(slots, ids, r["outgoing"], boxes, groups)
    K0, K1 = r["K0"], r["K1"]
    K0[W : W + fine.x, 0 : fine.y, 0:128] = coef[...]
    for i in range(mid.x):
        r["pairs"][i] = coef[2 * i] + coef[2 * i + 1]
    K1[W : W + mid.x, 0 : mid.y, :] = coarse_mid(r["pairs"], fine.x, fine.y)
    for i in range(mid.x // 2):
        r["pairsm"][i] = K1[W + 2 * i, 0 : mid.y, :] + K1[W + 2 * i + 1, 0 : mid.y, :]
    here = (at["gx"], at["gy"], at["gz"])
    coarse_low(r["pairsm"], mid.x // 2, mid.y, mid.z // 2, r["tmp"], r["gk"].at[here])
    pl.semaphore_wait(barrier, expected + len(others))

    moves = []
    me = at["gz"]
    for k in range(1, groups):
        to, source = lax.rem(me + k, groups), lax.rem(me + groups - k, groups)
        copy = pltpu.make_async_remote_copy(
            r["outgoing"].at[to], r["incoming"].at[me], r["ms"].at[k - 1], r["mr"].at[k - 1],
            device_id={"gz": to}, device_id_type=MESH)
        copy.start()
        arrive = pltpu.make_async_remote_copy(
            r["outgoing"].at[to], r["incoming"].at[source], r["ms"].at[k - 1], r["mr"].at[k - 1],
            device_id={"gz": to}, device_id_type=MESH)
        moves.append((copy, arrive))
    r["incoming"][me] = r["outgoing"][me]

    def bufs(n, tail):
        return tuple(r[b + tail].at[n] for b in ("py", "ly", "pz", "lz", "es", "er"))

    fine_halo, mid_halo = exchange(fine, K0, bufs(0, ""), counts), exchange(mid, K1, bufs(0, "m"), counts)
    low_gather = gather(r["gk"], r["gs"].at[0], r["gr"].at[0], counts)
    for step in (fine_halo, mid_halo, low_gather):
        next(step)
    lane = iota((BOX * BOX, 128), 1)
    folded = iota((BOX * BOX, 128), 0) % BOX == lane % BOX
    for b in range(boxes):
        block = jnp.where(folded & (lane // BOX == b), 1.0, 0.0)
        r["rhs"][BOX * BOX * b : BOX * BOX * (b + 1), :] = block.astype(jnp.bfloat16)
    for copy, arrive in moves:
        copy.wait_send()
        arrive.wait_recv()
    source = place_boxes(r["incoming"], owner, r["lhs"], r["rhs"], boxes, groups)
    source = source.reshape(fine.x, fine.y, 128)
    drain(fine_halo)

    faces0 = (r["fx0"], r["fy0"], r["fz0"])
    faces1 = (r["fx1"], r["fy1"], r["fz1"])
    dd0, iv0, dd1, iv1 = r["dd0"], r["iv0"], r["dd1"], r["iv1"]
    v0, g0, v1, g1 = r["v0"], r["g0"], r["v1"], r["g1"]
    prepare(fine, K0, *faces0, dd0, iv0)
    parity = iota((fine.y, 128), 0) + iota((fine.y, 128), 1)
    for x in range(fine.x):
        red = (parity + x) % 2 == 0
        r["P0"][W + x, 0 : fine.y, 0:128] = jnp.where(red, source[x] * iv0[W + x, 0 : fine.y, 0:128], source[x])
    step = exchange(fine, r["P0"], bufs(1, ""), counts)
    next(step)
    drain(mid_halo)
    prepare(mid, K1, *faces1, dd1, iv1)
    next(low_gather)
    drain(step)
    open_halo(fine, r["P0"], v0, g0, dd0)
    for reach, colour in ((3, 1), (2, 0), (1, 1)):
        half_sweep(fine, v0, g0, faces0, iv0, colour, reach)
    residual_pairs(fine, v0, g0, faces0, dd0, r["pairs"])

    source1 = coarse_mid(r["pairs"], fine.x, fine.y)
    parity = iota((mid.y, 128), 0) + iota((mid.y, 128), 1)
    for x in range(mid.x):
        red = (parity + x) % 2 == 0
        scaled = 4.0 * source1[x]
        r["P1"][W + x, 0 : mid.y, :] = jnp.where(red, scaled * iv1[W + x, 0 : mid.y, :], scaled)
    step = exchange(mid, r["P1"], bufs(1, "m"), counts)
    next(step)
    drain(low_gather)
    spread_low(r["gk"], r["k2"], counts, 1)
    drain(step)
    open_halo(mid, r["P1"], v1, g1, dd1)
    for reach, colour in ((3, 1), (2, 0), (1, 1)):
        half_sweep(mid, v1, g1, faces1, iv1, colour, reach)
    residual_pairs(mid, v1, g1, faces1, dd1, r["pairsm"])
    for i in range(mid.x // 2):
        r["pairsm"][i] = r["pairsm"][i] * 0.25
    coarse_low(r["pairsm"], mid.x // 2, mid.y, mid.z // 2, r["tmp"], r["gf"].at[here])
    r["E1"][W : W + mid.x, 0 : mid.y, :] = v1[W : W + mid.x, 0 : mid.y, :]
    drain(
        gather(r["gf"], r["gs"].at[1], r["gr"].at[1], counts),
        exchange(mid, r["E1"], bufs(2, "m"), counts))

    planes, rows, lanes = 4 * counts["gx"], 4 * counts["gy"], 32 * counts["gz"]
    spread_low(r["gf"], r["f2"], counts, 1)
    bottom(r["f2"], r["k2"], r["s2"], r["v2"], r["x2"], (planes, rows, lanes))
    row8 = iota((8, lanes), 0)
    for q in range(8):
        plane = r["x2"][4 * at["gx"] + q]
        turned = plane
        for c in range(1, counts["gy"]):
            turned = jnp.where(at["gy"] == c, pltpu.roll(plane, rows - 4 * c, 0), turned)
        r["local"][q] = jnp.where(row8 < 6, turned[0:8, :], turned[rows - 8 : rows, :])
    goal = iota((lanes, 128), 1)
    cell = jnp.where(goal < mid.z + W, goal, goal - 128)
    cell = (cell + 128) // 2 - 64
    wanted = (goal < mid.z + W) | (goal >= 128 - W)
    matrix = jnp.where((iota((lanes, 128), 0) == 32 * at["gz"] + cell) & wanted, 1.0, 0.0).astype(F32)
    spread = dot(r["local"][...].reshape(64, lanes), matrix).reshape(8, 8, 128)
    E1 = r["E1"]
    for q in range(8):
        r["wide"][pl.ds(0, 8, stride=2), :] = spread[q]
        r["wide"][pl.ds(1, 8, stride=2), :] = spread[q]
        for k in range(2):
            x = 2 * q + k
            E1[x] = jnp.where(K1[x] > 0.0, E1[x] + r["wide"][...], 0.0)
    for reach, colour in ((3, 0), (2, 1), (1, 0), (0, 1)):
        half_sweep(mid, E1, g1, faces1, iv1, colour, reach)

    matrix = jnp.where(iota((128, 128), 0) == iota((128, 128), 1) // 2, 1.0, 0.0).astype(F32)
    fresh = dot(E1[W : W + mid.x, 0 : mid.y, :].reshape(mid.x * mid.y, 128), matrix).reshape(mid.x, mid.y, 128)
    Q0 = r["Q0"]
    for i in range(mid.x):
        r["wide"][pl.ds(0, mid.y, stride=2), :] = fresh[i]
        r["wide"][pl.ds(1, mid.y, stride=2), :] = fresh[i]
        for k in range(2):
            x = W + 2 * i + k
            Q0[x, 0 : fine.y, 0:128] = v0[x, 0 : fine.y, 0:128] + r["wide"][...]
    drain(exchange(fine, Q0, bufs(2, ""), counts))
    for reach, colour in ((3, 0), (2, 1), (1, 0), (0, 1)):
        half_sweep(fine, Q0, g0, faces0, iv0, colour, reach)
    out[...] = Q0[W : W + fine.x, 0 : fine.y, 0:128]


def per_device(counts, old_slots, old_ids, old_owner, coefficient):
    x, y, z = coefficient.shape
    fine, mid = Level(x, y, z), Level(x // 2, y // 2, z // 2)
    planes, rows, lanes = 4 * counts["gx"], 4 * counts["gy"], 32 * counts["gz"]
    groups, boxes = counts["gz"], z // BOX
    cells = old_slots.shape[3]
    partners = counts["gx"] - 1 + counts["gy"] * groups - 1
    vmem = lambda *shape: pltpu.VMEM(shape, F32)
    dma = lambda *shape: pltpu.SemaphoreType.DMA(shape)
    scratch = {}
    for level, tail, names in ((fine, "", ("K0", "P0", "Q0")), (mid, "m", ("K1", "P1", "E1"))):
        for name in names:
            scratch[name] = vmem(*level.shape)
        scratch["py" + tail] = vmem(3, 2, level.x, W, 128)
        scratch["ly" + tail] = vmem(3, 2, level.xe, W, 128)
        scratch["pz" + tail] = vmem(3, level.y, 128)
        scratch["lz" + tail] = vmem(3, 2, 3, 3, level.y, 128)
        scratch["es" + tail] = dma(3, len(NEAR))
        scratch["er" + tail] = dma(3, len(NEAR))
        scratch["pairs" + tail] = vmem(level.x // 2, level.y, 128)
    for level, tail in ((fine, "0"), (mid, "1")):
        for name in ("fx", "fy", "fz", "dd", "iv", "v", "g"):
            scratch[name + tail] = vmem(*level.shape)
    scratch.update(
        outgoing=vmem(groups, SEND, cells), incoming=vmem(groups, SEND, cells), ms=dma(groups - 1), mr=dma(groups - 1),
        lhs=pltpu.VMEM((BOX * BOX, boxes * BOX * BOX), jnp.bfloat16),
        rhs=pltpu.VMEM((boxes * BOX * BOX, 128), jnp.bfloat16),
        tmp=vmem(mid.y, 128), wide=vmem(16, 128), local=vmem(8, 8, lanes),
        gk=vmem(counts["gx"], counts["gy"], groups, 8, 128), gf=vmem(counts["gx"], counts["gy"], groups, 8, 128),
        gs=dma(2, partners), gr=dma(2, partners),
        f2=vmem(planes + 2, rows, lanes), k2=vmem(planes + 2, rows, lanes), s2=vmem(planes + 2, rows, lanes),
        v2=vmem(planes, rows, lanes), x2=vmem(planes + 4, rows, lanes))
    return pl.pallas_call(
        functools.partial(kernel, fine, mid, counts, tuple(scratch)),
        out_shape=jax.ShapeDtypeStruct(coefficient.shape, F32),
        in_specs=[pl.BlockSpec(memory_space=pltpu.VMEM)] * 4,
        out_specs=pl.BlockSpec(memory_space=pltpu.VMEM),
        scratch_shapes=list(scratch.values()),
        compiler_params=pltpu.CompilerParams(
            collective_id=0, has_side_effects=True, vmem_limit_bytes=60 * 1024 * 1024),
    )(old_slots, old_ids, old_owner, coefficient)


def solution(mesh):
    counts = {axis: mesh.shape[axis] for axis in ("gx", "gy", "gz")}
    return jax.shard_map(
        functools.partial(per_device, counts), mesh=mesh,
        in_specs=(P("gx", "gy", "gz", None), P("gx", "gy", "gz"), P("gx", "gy", None), P("gx", "gy", "gz")),
        out_specs=P("gx", "gy", "gz"), check_vma=False)
```
